32 devices in a mesh: hi: 4 (over y, core), lo: 8 (over z, x).
Axes of the slice: x: 2, y: 2, z: 4, core: 2. Of those that a mesh axis runs over, the one named last changes fastest.
Arguments:
- grm: bfloat16 [4, 8, 64, 4, 512], P(None, 'lo', None, 'hi'), as said below
- right_sides: float32 [2048, 512], P(('hi', 'lo')), may hold values from -6 to 6
- inv_diag: float32 [2048], P(('hi', 'lo')), may hold values from 0.3 to 1
- bases: float32 [2048, 576], P(('hi', 'lo')), may hold values from -0.75 to 0.75
- couplings: float32 [9, 64, 64], replicated, as said below
- level_map: int32 [8], replicated, may hold values from 0 to 7, each once
- variance: float32 [2], replicated, may hold values from 0.3 to 1.5
- iters_per_column: int32 [512], replicated, may hold values from 1 to 3
Outputs:
- solution: float32 [2048, 512], P(('hi', 'lo'))
- residual: float32 [2048, 512], P(('hi', 'lo'))
The draws below stay inside these ranges and needn't reach their ends.
Inputs may be any that keep to these rules, and one draw needn't show every extreme that they name: `grm`: G is symmetric and positive definite. `couplings`: each of the 9 matrices is symmetric and positive definite. `level_map`: a permutation of the levels.
All inputs are finite; a program needn't handle non-finite values.
Results may differ from the reference program's by a relative error of at most 0.0055.
Values may be sent and summed in bfloat16 or wider, within the bound.
A program may use at most 64 MiB of HBM per device.

```python
import math
import jax
import jax.numpy as jnp
from jax import lax

ROWS_DEV = 64
RHS = 512
RANK = 64
LEVELS = 8
ITERS = 3
HI_BLOCKS = 4
LO_BLOCKS = 8
SAMPLES = 2048
N_HI = 4
N_LO = 8


def draw_grm(key, part):
    entries = jax.random.normal(key, (SAMPLES, SAMPLES), jnp.float32)
    spread = 0.45 / math.sqrt(2.0 * SAMPLES)
    symmetric = (entries + entries.T) * spread + jnp.eye(SAMPLES, dtype=jnp.float32)
    return symmetric.astype(jnp.bfloat16).reshape(HI_BLOCKS, LO_BLOCKS, ROWS_DEV, HI_BLOCKS, LO_BLOCKS * ROWS_DEV)


def draw_couplings(key, part):
    factors = jax.random.normal(jax.random.fold_in(key, 11), (LEVELS + 1, RANK, RANK), jnp.float32)
    low_end = math.log(0.3)
    high_end = math.log(1.0)
    level_scale = jnp.exp(jax.random.uniform(jax.random.fold_in(key, 12), (LEVELS + 1,), jnp.float32, low_end, high_end))
    gram = jnp.einsum('lij,lkj->lik', factors, factors, precision=lax.Precision.HIGHEST) / RANK
    gram = gram + 0.25 * jnp.eye(RANK, dtype=jnp.float32)[None]
    return gram * level_scale[:, None, None]


def place_ends(result, rng, least, high):
    index_at = [jax.random.randint(jax.random.fold_in(rng, axis), (), 0, length) for axis, length in enumerate(result.shape)]
    widest = result.shape.index(max(result.shape))
    beside = index_at[:widest] + [(index_at[widest] + 1) % result.shape[widest]] + index_at[widest + 1:]
    return result.at[tuple(index_at)].set(least).at[tuple(beside)].set(high)


def block_scale(key, dims, cuts, smallest, top_value):
    level, own = 1.0, jax.random.fold_in(key, 6)
    for position, shards_of in cuts:
        steps = jnp.exp(jax.random.uniform(jax.random.fold_in(own, position), (shards_of,), jnp.float32, smallest / len(cuts), top_value / len(cuts)))
        level = level * jnp.repeat(steps, dims[position] // shards_of).reshape([-1 if axis == position else 1 for axis in range(len(dims))])
    return level


def noise(stream_key, dims, scale, most, cuts=(), held_as=jnp.bfloat16):
    gain = block_scale(stream_key, dims, cuts, -0.22, 0.18) if cuts else 1.0
    values = jax.random.normal(stream_key, dims, jnp.float32) * scale * gain
    return jnp.minimum(jnp.maximum(values, -most), most).astype(held_as)


def setup_inputs(seed: int = 0) -> dict:
    key_of = jax.random.split(jax.random.key(seed), 9)
    return {
        "grm": draw_grm(jax.random.fold_in(key_of[8], 71), 0),
        "right_sides": noise(key_of[1], (SAMPLES, RHS), 1.0, 6.0, ((0, 32),), jnp.float32),
        "inv_diag": jnp.clip(jnp.exp(math.log(1.0) - 1.2039728 * jax.random.uniform(key_of[2], (SAMPLES,), jnp.float32) ** block_scale(key_of[2], (SAMPLES,), ((0, 32),), -0.2, 0.2)), 0.3, 1.0),
        "bases": noise(key_of[3], (SAMPLES, (LEVELS + 1) * RANK), ROWS_DEV ** -0.5, 0.75, ((0, 32),), jnp.float32),
        "couplings": draw_couplings(jax.random.fold_in(key_of[8], 71), 0),
        "level_map": jax.random.permutation(key_of[5], LEVELS).astype(jnp.int32),
        "variance": jnp.clip(jnp.exp(jax.random.uniform(key_of[6], (2,), jnp.float32, math.log(0.3), math.log(1.5))), 0.3, 1.5),
        "iters_per_column": place_ends(jax.random.randint(key_of[7], (RHS,), 1, ITERS + 1), jax.random.fold_in(key_of[7], 1), 1, ITERS).astype(jnp.int32),
    }


def apply_system(grm, direction, variance):
    matrix = grm.reshape(SAMPLES, SAMPLES)
    product = jnp.dot(matrix, direction.astype(jnp.bfloat16), preferred_element_type=jnp.float32)
    return variance[0] * product + variance[1] * direction


def precondition(resid, inv_diag, bases, couplings, level_map):
    blocks = N_HI * N_LO
    bit_count = blocks.bit_length() - 1
    level_total = LEVELS + 1
    resid_blocks = resid.reshape(blocks, ROWS_DEV, RHS)
    basis_blocks = bases.reshape(blocks, ROWS_DEV, level_total * RANK)
    coefficients = jnp.einsum("dnk,dnb->dkb", basis_blocks, resid_blocks, precision=lax.Precision.HIGHEST)
    coefficients = coefficients.reshape(blocks, level_total, RANK, RHS)
    stacked = jnp.zeros_like(coefficients)
    order = jnp.arange(blocks, dtype=jnp.int32)
    level_ids = jnp.arange(level_total, dtype=jnp.int32)
    for bit_index in range(bit_count):
        level = level_map[bit_index]
        partner = jnp.bitwise_xor(order, 1 << bit_index).astype(jnp.int32)
        chosen = jnp.take(coefficients, level, axis=1)
        summed = chosen + jnp.take(chosen, partner, axis=0)
        matrix = jnp.take(couplings, level, axis=0)
        term = jnp.einsum("rs,dsb->drb", matrix, summed, precision=lax.Precision.HIGHEST)
        select = (level_ids == level).astype(jnp.float32)
        stacked = stacked + select[None, :, None, None] * term[:, None]
    total = jnp.sum(coefficients[:, LEVELS], axis=0)
    coarse = jnp.dot(couplings[LEVELS], total, precision=lax.Precision.HIGHEST)
    stacked = stacked.at[:, LEVELS].add(coarse[None])
    lifted = jnp.einsum("dnk,dkb->dnb", basis_blocks, stacked.reshape(blocks, level_total * RANK, RHS), precision=lax.Precision.HIGHEST)
    return inv_diag[:, None] * resid + lifted.reshape(SAMPLES, RHS)


def reference(grm, right_sides, inv_diag, bases, couplings, level_map, variance, iters_per_column):
    solution = jnp.zeros_like(right_sides)
    residual = right_sides
    scaled = precondition(residual, inv_diag, bases, couplings, level_map)
    direction = scaled
    energy = jnp.sum(residual * scaled, axis=0)
    for step in range(ITERS):
        image = apply_system(grm, direction, variance)
        curvature = jnp.sum(direction * image, axis=0)
        alpha = energy / curvature
        stepsize = jnp.where(step < iters_per_column, alpha, jnp.zeros_like(alpha))
        solution = solution + stepsize * direction
        residual = residual - stepsize * image
        if step + 1 < ITERS:
            scaled = precondition(residual, inv_diag, bases, couplings, level_map)
            fresh = jnp.sum(residual * scaled, axis=0)
            direction = scaled + (fresh / energy) * direction
            energy = fresh
    return solution, residual
```

```python
import functools

import jax
import jax.numpy as jnp
from jax import lax
from jax.experimental import pallas as pl
from jax.experimental.pallas import tpu as pltpu
from jax.sharding import PartitionSpec as P

ITERS = 3
MESH = pl.DeviceIdType.MESH


def from_partner(value, axis, bit):
    mask = 2**bit
    pairs = [(source, source ^ mask) for source in range(lax.axis_size(axis))]
    return lax.ppermute(value, axis, pairs)


def level_pieces(coefficients, couplings, level):
    level_ids = jnp.arange(couplings.shape[0], dtype=jnp.int32)
    select = (level_ids == level).astype(jnp.float32)
    own_part = jnp.einsum("l,lrb->rb", select, coefficients)
    matrix = jnp.einsum("l,lrs->rs", select, couplings)
    return (own_part, matrix, select)


def add_level(stacked, own_part, other_part, matrix, select):
    term = jnp.dot(matrix, own_part + other_part, precision=lax.Precision.HIGHEST)
    return stacked + select[:, None, None] * term[None]


def local(grm, right_sides, inv_diag, bases, couplings, level_map, variance, iters_per_column):
    row_count, column_count = right_sides.shape
    grm_block = grm.reshape(-1, grm.shape[4])
    level_total = couplings.shape[0]
    rank_width = couplings.shape[1]
    lo_bits = lax.axis_size("lo").bit_length() - 1
    hi_bits = lax.axis_size("hi").bit_length() - 1
    genetic = variance[0]
    noise = variance[1]

    def precondition(resid):
        coefficients = lax.dot_general(
            bases, resid, (((0,), (0,)), ((), ())), precision=lax.Precision.HIGHEST
        )
        coefficients = coefficients.reshape(level_total, rank_width, column_count)
        stacked = jnp.zeros((level_total - 1, rank_width, column_count), jnp.float32)
        for bit_index in range(lo_bits):
            own_part, matrix, select = level_pieces(coefficients, couplings, level_map[bit_index])
            other_part = from_partner(own_part.astype(jnp.bfloat16), "lo", bit_index).astype(
                own_part.dtype
            )
            stacked = add_level(stacked, own_part, other_part, matrix, select[: level_total - 1])
        for bit_index in range(hi_bits):
            own_part, matrix, select = level_pieces(
                coefficients, couplings, level_map[lo_bits + bit_index]
            )
            other_part = from_partner(own_part.astype(jnp.bfloat16), "hi", bit_index).astype(
                own_part.dtype
            )
            stacked = add_level(stacked, own_part, other_part, matrix, select[: level_total - 1])
        split_at = (level_total - 1) * rank_width
        local_part = inv_diag[:, None] * resid + jnp.dot(
            bases[:, :split_at],
            stacked.reshape(split_at, column_count),
            precision=lax.Precision.HIGHEST,
        )
        coarse_basis = bases[:, split_at:]
        partial_energy = jnp.sum(resid * local_part, axis=0)
        total, summed_energy = lax.psum(
            (coefficients[level_total - 1], partial_energy), ("hi", "lo")
        )
        coarse = jnp.dot(couplings[level_total - 1], total, precision=lax.Precision.HIGHEST)
        scaled = local_part + jnp.dot(coarse_basis, coarse, precision=lax.Precision.HIGHEST)
        energy = summed_energy + jnp.sum(total * coarse, axis=0)
        return (scaled, energy)

    solution = jnp.zeros_like(right_sides)
    residual = right_sides
    scaled, energy = precondition(residual)
    direction = scaled
    for step in range(ITERS):
        rounded = direction.astype(jnp.bfloat16)
        partial_value = jnp.dot(
            grm_block,
            lax.all_gather(rounded, "lo", axis=0, tiled=True),
            preferred_element_type=jnp.float32,
        )
        product = lax.psum_scatter(partial_value, "hi", scatter_dimension=0, tiled=True)
        image = genetic * product + noise * direction
        curvature = lax.psum(jnp.sum(direction * image, axis=0), ("hi", "lo"))
        alpha = energy / curvature
        stepsize = jnp.where(step < iters_per_column, alpha, jnp.zeros_like(alpha))
        solution = solution + stepsize * direction
        residual = residual - stepsize * image
        if step + 1 < ITERS:
            scaled, fresh = precondition(residual)
            direction = scaled + fresh / energy * direction
            energy = fresh
    return (solution, residual)


def fits_one_device(mesh, grm, right_sides, bases, couplings):
    n_hi, n_lo = mesh.shape["hi"], mesh.shape["lo"]
    devices = n_hi * n_lo
    samples, columns = right_sides.shape
    rank = couplings.shape[1]
    bits = devices.bit_length() - 1
    used = (bits + 1) * rank
    width = samples // n_hi
    return (
        n_hi == 2 * CORES
        and n_lo % (2 * XDIM) == 0
        and columns % (16 * devices) == 0
        and columns // devices == 16
        and used % 128 == 0
        and (bits + 1) % 2 == 0
        and width % 256 == 0
        and 2 * rank == 128
        and 2 * (samples // devices) == 128
        and samples * (samples + used) * 2 < 2**24
    )


CORES = 2
XDIM = 2


def nt(a, b):
    return lax.dot_general(a, b, (((1,), (1,)), ((), ())), preferred_element_type=jnp.float32)


def nn(a, b):
    return jnp.dot(a, b, preferred_element_type=jnp.float32)


def halves(value, axis):
    top = value.astype(jnp.bfloat16)
    rest = (value - top.astype(jnp.float32)).astype(jnp.bfloat16)
    return jnp.concatenate([top, rest], axis=axis)


def whole_kernel(
    n_hi, n_lo,
    var_ref, level_ref,
    grm_ref, rhs_ref, inv_ref, bases_ref, coup_ref, iters_ref,
    sol_ref, res_ref,
    pay, xsend, xrecv, isend, irecv, osend, orecv,
    resid, direct, image, iterate, scaled, inv_row,
    coef, summed, lifted, couple,
    send_sem, recv_sem, side_send, side_recv,
):
    hi, lo = lax.axis_index("hi"), lax.axis_index("lo")
    n = n_hi * n_lo
    me = hi * n_lo + lo
    y, core = hi // CORES, hi % CORES
    z, x = lo // XDIM, lo % XDIM
    depth = n_lo // XDIM
    rows, columns = rhs_ref.shape
    mine = columns // n
    half = mine // 2
    levels = coup_ref.shape[0]
    rank = coup_ref.shape[1]
    bits = n.bit_length() - 1
    used = (bits + 1) * rank
    width = grm_ref.shape[2]
    quad = width // 2
    samples = rows * n
    f32, bf16 = jnp.float32, jnp.bfloat16

    barrier = pltpu.get_barrier_semaphore()

    def other(step):
        peer = lax.rem(me + step, n)
        return (peer // n_lo, lax.rem(peer, n_lo))

    def greet(step, carry):
        pl.semaphore_signal(barrier, inc=1, device_id=other(step), device_id_type=MESH)
        return carry

    lax.fori_loop(1, n, greet, 0)

    column_id = lax.broadcasted_iota(jnp.int32, (1, used), 1)
    wanted = jnp.full((1, used), (levels - 1) * rank, jnp.int32)
    for bit in range(bits):
        wanted = jnp.where(column_id // rank == bit, level_ref[bit] * rank, wanted)
    wanted = wanted + column_id % rank
    pick = lax.broadcasted_iota(jnp.int32, (levels * rank, used), 0) == wanted
    own_bases = nn(bases_ref[...].astype(bf16), pick.astype(f32).astype(bf16))
    lanes = (
        slice(0, used + quad),
        slice(used + quad, used + quad + width),
        slice(used + quad + width, used + quad + 2 * width),
    )
    pay[me, :, 0:used] = own_bases.astype(bf16)
    across = lax.rem(hi + CORES, n_hi)
    upper = jnp.where(hi < CORES, lo >= n_lo // 2, lo < n_lo // 2)
    both = grm_ref[across]
    pay[me, :, used : used + quad] = jnp.where(
        upper, both[:, quad:].astype(f32), both[:, :quad].astype(f32)
    ).astype(bf16)
    pay[me, :, lanes[1]] = grm_ref[hi]
    pay[me, :, lanes[2]] = grm_ref[lax.rem(hi + 1, n_hi)]

    turned = rhs_ref[...].T.reshape(n, mine, rows)
    xsend[...] = jnp.concatenate([turned[:, :half], turned[:, half:]], axis=2)
    isend[0, :, 0:rows] = inv_ref[...]
    isend[0, :, rows:] = inv_ref[...]

    couple[...] = jnp.zeros_like(couple)
    for bit in range(bits + 1):
        block = coup_ref[level_ref[bit]] if bit < bits else coup_ref[levels - 1]
        at = slice(bit * rank, (bit + 1) * rank)
        couple[0, at, at] = block.astype(bf16)
        couple[1, at, at] = (block - block.astype(bf16).astype(f32)).astype(bf16)
    taken = lax.broadcasted_iota(jnp.int32, (mine, columns), 1) == (
        me * mine + lax.broadcasted_iota(jnp.int32, (mine, columns), 0)
    )
    steps_wanted = jnp.sum(
        jnp.where(taken, iters_ref[...].astype(f32), 0.0), axis=1, keepdims=True
    )

    pl.semaphore_wait(barrier, n - 1)

    def exchange(source, target, kind):
        def send(step, carry):
            peer = lax.rem(me + step, n)
            pltpu.make_async_remote_copy(
                src_ref=source.at[peer], dst_ref=target.at[me],
                send_sem=side_send.at[kind], recv_sem=side_recv.at[kind],
                device_id=(peer // n_lo, lax.rem(peer, n_lo)), device_id_type=MESH,
            ).start()
            return carry

        lax.fori_loop(1, n, send, 0)
        target[me] = source[me]

    def settle(target, kind):
        all_but_one = target.at[pl.ds(0, n - 1)]
        pltpu.make_async_copy(all_but_one, all_but_one, side_recv.at[kind]).wait()

    def drain(source, kind):
        all_but_one = source.at[pl.ds(0, n - 1)]
        pltpu.make_async_copy(all_but_one, all_but_one, side_send.at[kind]).wait()

    def send_inv(step, carry):
        pltpu.make_async_remote_copy(
            src_ref=isend.at[0], dst_ref=irecv.at[me],
            send_sem=side_send.at[1], recv_sem=side_recv.at[1],
            device_id=other(step), device_id_type=MESH,
        ).start()
        return carry

    def forward(index, part, target_hi, target_lo):
        here = pay.at[index, :, lanes[part]]
        pltpu.make_async_remote_copy(
            src_ref=here, dst_ref=here,
            send_sem=send_sem.at[part], recv_sem=recv_sem.at[part, index],
            device_id=(target_hi, target_lo), device_id_type=MESH,
        ).start()

    def arrive(index, part):
        here = pay.at[index, :, lanes[part]]
        pltpu.make_async_copy(here, here, recv_sem.at[part, index]).wait()

    x_lo = lo + 1 - 2 * x
    y_hi = hi + CORES - 2 * CORES * y
    c_hi = hi + 1 - 2 * core

    def turned_z(step):
        return lax.rem(z + step, depth) * XDIM

    def send_own(part):
        forward(me, part, hi, x_lo)
        forward(me, part, y_hi, lo)
        for step in range(1, depth):
            forward(me, part, hi, turned_z(step) + x)
        forward(me, part, c_hi, lo)

    def by_x(part, step):
        return (part == 0) if part != 1 else (step % 2 == 0)

    def relay(part):
        for step in range(depth):
            own_column = hi * n_lo + turned_z(step) + x
            if step > 0:
                arrive(own_column, part)
                forward(own_column, part, hi, x_lo)
                forward(own_column, part, y_hi, lo)
                forward(own_column, part, c_hi, lo)
            beside_x = hi * n_lo + turned_z(step) + 1 - x
            arrive(beside_x, part)
            if by_x(part, step):
                forward(beside_x, part, y_hi, lo)
            forward(beside_x, part, c_hi, lo)
            beside_y = y_hi * n_lo + turned_z(step) + x
            arrive(beside_y, part)
            if not by_x(part, step):
                forward(beside_y, part, hi, x_lo)
            forward(beside_y, part, c_hi, lo)
        for step in range(depth):
            corner = y_hi * n_lo + turned_z(step) + 1 - x
            arrive(corner, part)
            forward(corner, part, c_hi, lo)

    def from_core(part):
        for own_y in (True, False):
            base = (c_hi if own_y else lax.rem(c_hi + CORES, n_hi)) * n_lo
            for block in range(n_lo):
                arrive(base + block, part)

    exchange(xsend, xrecv, 0)
    lax.fori_loop(1, n, send_inv, 0)
    irecv[me] = isend[0]
    for part in range(3):
        send_own(part)
    relay(0)
    from_core(0)
    settle(xrecv, 0)
    settle(irecv, 1)

    for pair in range(n // 2):
        at = slice(pair * 2 * rows, (pair + 1) * 2 * rows)
        one, two = xrecv[2 * pair], xrecv[2 * pair + 1]
        resid[0:half, at] = jnp.concatenate([one[:, :rows], two[:, :rows]], axis=1)
        resid[half:mine, at] = jnp.concatenate([one[:, rows:], two[:, rows:]], axis=1)
        low = lax.broadcasted_iota(jnp.int32, (1, 2 * rows), 1) < rows
        inv_row[:, at] = jnp.where(low, irecv[2 * pair], irecv[2 * pair + 1])

    group = n // 4
    span = group * rows

    def precondition():
        def down(q, carry):
            part = halves(resid[:, pl.ds(pl.multiple_of(q * span, span), span)], 0)
            for j in range(group):
                both = nn(part[:, j * rows : (j + 1) * rows], pay[q * group + j, :, 0:used])
                coef[q * group + j] = both[:mine] + both[mine:]
            return carry

        lax.fori_loop(0, n // group, down, 0)
        low = lax.broadcasted_iota(jnp.int32, (mine, 2 * rank), 1) < rank
        for chunk in range(used // (2 * rank)):
            at = slice(chunk * 2 * rank, (chunk + 1) * 2 * rank)
            first, second = 2 * chunk, 2 * chunk + 1
            if second == bits:
                total = coef[0, :, at]
                for k in range(1, n):
                    total = total + coef[k, :, at]
            for k in range(n):
                own = coef[k, :, at]
                left = own + coef[k ^ (1 << first), :, at]
                right = total if second == bits else own + coef[k ^ (1 << second), :, at]
                summed[k, :, at] = halves(jnp.where(low, left, right), 0)
        both = nn(summed[...].reshape(n * 2 * mine, used), couple[0]).reshape(n, 2 * mine, used)
        rest = nn(summed[:, :mine].reshape(n * mine, used), couple[1]).reshape(n, mine, used)
        lifted[...] = halves(both[:, :mine] + both[:, mine:] + rest, 1)

        def up(q, carry):
            pieces = []
            for j in range(group):
                both = nt(lifted[q * group + j], pay[q * group + j, :, 0:used])
                pieces.append(both[:mine] + both[mine:])
            at = pl.ds(pl.multiple_of(q * span, span), span)
            scaled[:, at] = inv_row[:, at] * resid[:, at] + jnp.concatenate(pieces, axis=1)
            return carry

        lax.fori_loop(0, n // group, up, 0)
        return jnp.sum(resid[...] * scaled[...], axis=1, keepdims=True)

    def apply_grm():
        cut = [direct[:, h * width : (h + 1) * width].astype(bf16) for h in range(n_hi)]
        total = [jnp.zeros((mine, width), f32) for _ in range(n_hi)]
        for h in range(n_hi):
            near, far = (h + 1) % n_hi, (h + 2) % n_hi
            base = h * n_lo
            full = pay[base : base + n_lo, :, lanes[1]].reshape(width, width)
            total[h] = total[h] + nn(cut[h], full)
            full = pay[base : base + n_lo, :, lanes[2]].reshape(width, width)
            total[h] = total[h] + nn(cut[near], full)
            total[near] = total[near] + nt(cut[h], full)
            sums = {}
            for r in range(2):
                q = r if h < CORES else 1 - r
                blocks = pay[
                    base + r * (n_lo // 2) : base + (r + 1) * (n_lo // 2), :, used : used + quad
                ].reshape(quad, quad)
                sums["h", q] = nn(cut[far][:, r * quad : (r + 1) * quad], blocks)
                sums["far", r] = nt(cut[h][:, q * quad : (q + 1) * quad], blocks)
            total[h] = total[h] + jnp.concatenate([sums["h", 0], sums["h", 1]], axis=1)
            total[far] = total[far] + jnp.concatenate([sums["far", 0], sums["far", 1]], axis=1)
        for h in range(n_hi):
            at = slice(h * width, (h + 1) * width)
            image[:, at] = var_ref[0] * total[h] + var_ref[1] * direct[:, at]

    energy = precondition()
    direct[...] = scaled[...]
    iterate[...] = jnp.zeros_like(iterate)
    for part in (1, 2):
        relay(part)
        from_core(part)
    for step in range(ITERS):
        apply_grm()
        curvature = jnp.sum(direct[...] * image[...], axis=1, keepdims=True)
        alpha = jnp.where(steps_wanted > step, energy / curvature, 0.0)
        iterate[...] = iterate[...] + alpha * direct[...]
        resid[...] = resid[...] - alpha * image[...]
        if step + 1 < ITERS:
            fresh = precondition()
            direct[...] = scaled[...] + (fresh / energy) * direct[...]
            energy = fresh

    for which, field in ((0, iterate), (1, resid)):
        for pair in range(n // 2):
            both = field[:, pair * 2 * rows : (pair + 1) * 2 * rows]
            top, bottom = both[:half], both[half:]
            osend[2 * pair, which] = jnp.concatenate([top[:, :rows], bottom[:, :rows]], axis=1)
            osend[2 * pair + 1, which] = jnp.concatenate([top[:, rows:], bottom[:, rows:]], axis=1)
    exchange(osend, orecv, 2)
    for part in range(3):
        sent = pay.at[pl.ds(0, n - 1), :, lanes[part]]
        pltpu.make_async_copy(sent, sent, send_sem.at[part]).wait()
    drain(xsend, 0)
    drain(irecv, 1)
    settle(orecv, 2)
    for which, out_ref in ((0, sol_ref), (1, res_ref)):
        got = orecv[:, which]
        apart = jnp.concatenate([got[:, :, :rows], got[:, :, rows:]], axis=1)
        out_ref[...] = apart.reshape(columns, rows).T
    drain(osend, 2)


def run_whole(mesh, grm, right_sides, inv_diag, bases, couplings, level_map, variance, iters):
    n_hi, n_lo = mesh.shape["hi"], mesh.shape["lo"]
    n = n_hi * n_lo
    rows, columns = right_sides.shape
    mine = columns // n
    rank = couplings.shape[1]
    used = n.bit_length() * rank
    width = grm.shape[4]
    samples = rows * n
    f32, bf16 = jnp.float32, jnp.bfloat16
    vmem = pl.BlockSpec(memory_space=pltpu.VMEM)
    smem = pl.BlockSpec(memory_space=pltpu.SMEM)
    field = pltpu.VMEM((mine, samples), f32)
    tile = (mine // 2, 2 * rows)
    return pl.pallas_call(
        functools.partial(whole_kernel, n_hi, n_lo),
        out_shape=(jax.ShapeDtypeStruct((rows, columns), f32),) * 2,
        in_specs=[smem, smem] + [vmem] * 6,
        out_specs=(vmem, vmem),
        scratch_shapes=[
            pltpu.VMEM((n, rows, used + width // 2 + 2 * width), bf16),
            pltpu.VMEM((n,) + tile, f32),
            pltpu.VMEM((n,) + tile, f32),
            pltpu.VMEM((1, 1, 2 * rows), f32),
            pltpu.VMEM((n, 1, 2 * rows), f32),
            pltpu.VMEM((n, 2) + tile, f32),
            pltpu.VMEM((n, 2) + tile, f32),
            field, field, field, field, field,
            pltpu.VMEM((1, samples), f32),
            pltpu.VMEM((n, mine, used), f32),
            pltpu.VMEM((n, 2 * mine, used), bf16),
            pltpu.VMEM((n, 2 * mine, used), bf16),
            pltpu.VMEM((2, used, used), bf16),
            pltpu.SemaphoreType.DMA((3,)),
            pltpu.SemaphoreType.DMA((3, n)),
            pltpu.SemaphoreType.DMA((3,)),
            pltpu.SemaphoreType.DMA((3,)),
        ],
        compiler_params=pltpu.CompilerParams(
            collective_id=0, has_side_effects=True, vmem_limit_bytes=56 * 2**20
        ),
    )(
        variance, level_map,
        grm.reshape(grm.shape[0], rows, width), right_sides, inv_diag.reshape(1, rows),
        bases, couplings, iters.reshape(1, columns),
    )


def solution(mesh):
    in_specs = (
        P(None, "lo", None, "hi", None),
        P(("hi", "lo"), None),
        P(("hi", "lo")),
        P(("hi", "lo"), None),
        P(),
        P(),
        P(),
        P(),
    )
    out_specs = (P(("hi", "lo"), None), P(("hi", "lo"), None))

    def program(*arrays):
        body = local
        if fits_one_device(mesh, arrays[0], arrays[1], arrays[3], arrays[4]):
            body = functools.partial(run_whole, mesh)
        return jax.shard_map(
            body, mesh=mesh, in_specs=in_specs, out_specs=out_specs, check_vma=False
        )(*arrays)

    return program
```

```python
import functools

import jax
import jax.numpy as jnp
from jax import lax
from jax.experimental import pallas as pl
from jax.experimental.pallas import tpu as pltpu
from jax.sharding import PartitionSpec as P

ITERS = 3
MESH = pl.DeviceIdType.MESH


def from_partner(value, axis, bit):
    mask = 2**bit
    pairs = [(source, source ^ mask) for source in range(lax.axis_size(axis))]
    return lax.ppermute(value, axis, pairs)


def level_pieces(coefficients, couplings, level):
    level_ids = jnp.arange(couplings.shape[0], dtype=jnp.int32)
    select = (level_ids == level).astype(jnp.float32)
    own_part = jnp.einsum("l,lrb->rb", select, coefficients)
    matrix = jnp.einsum("l,lrs->rs", select, couplings)
    return (own_part, matrix, select)


def add_level(stacked, own_part, other_part, matrix, select):
    term = jnp.dot(matrix, own_part + other_part, precision=lax.Precision.HIGHEST)
    return stacked + select[:, None, None] * term[None]


def local(grm, right_sides, inv_diag, bases, couplings, level_map, variance, iters_per_column):
    row_count, column_count = right_sides.shape
    grm_block = grm.reshape(-1, grm.shape[4])
    level_total = couplings.shape[0]
    rank_width = couplings.shape[1]
    lo_bits = lax.axis_size("lo").bit_length() - 1
    hi_bits = lax.axis_size("hi").bit_length() - 1
    genetic = variance[0]
    noise = variance[1]

    def precondition(resid):
        coefficients = lax.dot_general(
            bases, resid, (((0,), (0,)), ((), ())), precision=lax.Precision.HIGHEST
        )
        coefficients = coefficients.reshape(level_total, rank_width, column_count)
        stacked = jnp.zeros((level_total - 1, rank_width, column_count), jnp.float32)
        for bit_index in range(lo_bits):
            own_part, matrix, select = level_pieces(coefficients, couplings, level_map[bit_index])
            other_part = from_partner(own_part.astype(jnp.bfloat16), "lo", bit_index).astype(
                own_part.dtype
            )
            stacked = add_level(stacked, own_part, other_part, matrix, select[: level_total - 1])
        for bit_index in range(hi_bits):
            own_part, matrix, select = level_pieces(
                coefficients, couplings, level_map[lo_bits + bit_index]
            )
            other_part = from_partner(own_part.astype(jnp.bfloat16), "hi", bit_index).astype(
                own_part.dtype
            )
            stacked = add_level(stacked, own_part, other_part, matrix, select[: level_total - 1])
        split_at = (level_total - 1) * rank_width
        local_part = inv_diag[:, None] * resid + jnp.dot(
            bases[:, :split_at],
            stacked.reshape(split_at, column_count),
            precision=lax.Precision.HIGHEST,
        )
        coarse_basis = bases[:, split_at:]
        partial_energy = jnp.sum(resid * local_part, axis=0)
        total, summed_energy = lax.psum(
            (coefficients[level_total - 1], partial_energy), ("hi", "lo")
        )
        coarse = jnp.dot(couplings[level_total - 1], total, precision=lax.Precision.HIGHEST)
        scaled = local_part + jnp.dot(coarse_basis, coarse, precision=lax.Precision.HIGHEST)
        energy = summed_energy + jnp.sum(total * coarse, axis=0)
        return (scaled, energy)

    solution = jnp.zeros_like(right_sides)
    residual = right_sides
    scaled, energy = precondition(residual)
    direction = scaled
    for step in range(ITERS):
        rounded = direction.astype(jnp.bfloat16)
        partial_value = jnp.dot(
            grm_block,
            lax.all_gather(rounded, "lo", axis=0, tiled=True),
            preferred_element_type=jnp.float32,
        )
        product = lax.psum_scatter(partial_value, "hi", scatter_dimension=0, tiled=True)
        image = genetic * product + noise * direction
        curvature = lax.psum(jnp.sum(direction * image, axis=0), ("hi", "lo"))
        alpha = energy / curvature
        stepsize = jnp.where(step < iters_per_column, alpha, jnp.zeros_like(alpha))
        solution = solution + stepsize * direction
        residual = residual - stepsize * image
        if step + 1 < ITERS:
            scaled, fresh = precondition(residual)
            direction = scaled + fresh / energy * direction
            energy = fresh
    return (solution, residual)


def fits_one_device(mesh, grm, right_sides, bases, couplings):
    n_hi, n_lo = mesh.shape["hi"], mesh.shape["lo"]
    devices = n_hi * n_lo
    samples, columns = right_sides.shape
    rank = couplings.shape[1]
    bits = devices.bit_length() - 1
    used = (bits + 1) * rank
    width = samples // n_hi
    return (
        n_hi == 2 * CORES
        and n_lo % (2 * XDIM) == 0
        and columns % (16 * devices) == 0
        and columns // devices == 16
        and used % 128 == 0
        and (bits + 1) % 2 == 0
        and width % 256 == 0
        and 2 * rank == 128
        and 2 * (samples // devices) == 128
        and samples * (samples + used) * 2 < 2**24
    )


CORES = 2
XDIM = 2
LAG = 4


def nt(a, b):
    return lax.dot_general(a, b, (((1,), (1,)), ((), ())), preferred_element_type=jnp.float32)


def nn(a, b):
    return jnp.dot(a, b, preferred_element_type=jnp.float32)


def halves(value, axis):
    top = value.astype(jnp.bfloat16)
    rest = (value - top.astype(jnp.float32)).astype(jnp.bfloat16)
    return jnp.concatenate([top, rest], axis=axis)


def whole_kernel(
    n_hi, n_lo,
    var_ref, level_ref,
    grm_ref, rhs_ref, inv_ref, bases_ref, coup_ref, iters_ref,
    sol_ref, res_ref,
    pay, near_pay, next_pay, xsend, xrecv, isend, irecv, osend, orecv,
    resid, direct, image, iterate, scaled, inv_row,
    coef, summed, lifted, couple,
    send_sem, recv_sem, side_send, side_recv,
):
    hi, lo = lax.axis_index("hi"), lax.axis_index("lo")
    n = n_hi * n_lo
    me = hi * n_lo + lo
    y, core = hi // CORES, hi % CORES
    z, x = lo // XDIM, lo % XDIM
    depth = n_lo // XDIM
    rows, columns = rhs_ref.shape
    mine = columns // n
    half = mine // 2
    levels = coup_ref.shape[0]
    rank = coup_ref.shape[1]
    bits = n.bit_length() - 1
    used = (bits + 1) * rank
    width = grm_ref.shape[2]
    quad = width // 2
    samples = rows * n
    f32, bf16 = jnp.float32, jnp.bfloat16

    barrier = pltpu.get_barrier_semaphore()

    def other(step):
        peer = lax.rem(me + step, n)
        return (peer // n_lo, lax.rem(peer, n_lo))

    def greet(step, carry):
        pl.semaphore_signal(barrier, inc=1, device_id=other(step), device_id_type=MESH)
        return carry

    lax.fori_loop(1, n, greet, 0)

    column_id = lax.broadcasted_iota(jnp.int32, (1, used), 1)
    wanted = jnp.full((1, used), (levels - 1) * rank, jnp.int32)
    for bit in range(bits):
        wanted = jnp.where(column_id // rank == bit, level_ref[bit] * rank, wanted)
    wanted = wanted + column_id % rank
    pick = lax.broadcasted_iota(jnp.int32, (levels * rank, used), 0) == wanted
    own_bases = nn(bases_ref[...].astype(bf16), pick.astype(f32).astype(bf16))
    parts = (pay, near_pay, next_pay)
    pay[me, :, 0:used] = own_bases.astype(bf16)
    across = lax.rem(hi + CORES, n_hi)
    upper = jnp.where(hi < CORES, lo >= n_lo // 2, lo < n_lo // 2)
    both = grm_ref[across]
    pay[me, :, used : used + quad] = jnp.where(
        upper, both[:, quad:].astype(f32), both[:, :quad].astype(f32)
    ).astype(bf16)
    near_pay[me] = grm_ref[hi]
    next_pay[me] = grm_ref[lax.rem(hi + 1, n_hi)]

    turned = rhs_ref[...].T.reshape(n, mine, rows)
    xsend[...] = jnp.concatenate([turned[:, :half], turned[:, half:]], axis=2)
    isend[0, :, 0:rows] = inv_ref[...]
    isend[0, :, rows:] = inv_ref[...]

    couple[...] = jnp.zeros_like(couple)
    for bit in range(bits + 1):
        block = coup_ref[level_ref[bit]] if bit < bits else coup_ref[levels - 1]
        at = slice(bit * rank, (bit + 1) * rank)
        couple[0, at, at] = block.astype(bf16)
        couple[1, at, at] = (block - block.astype(bf16).astype(f32)).astype(bf16)
    taken = lax.broadcasted_iota(jnp.int32, (mine, columns), 1) == (
        me * mine + lax.broadcasted_iota(jnp.int32, (mine, columns), 0)
    )
    steps_wanted = jnp.sum(
        jnp.where(taken, iters_ref[...].astype(f32), 0.0), axis=1, keepdims=True
    )

    pl.semaphore_wait(barrier, n - 1)

    def exchange(source, target, kind):
        def send(step, carry):
            peer = lax.rem(me + step, n)
            pltpu.make_async_remote_copy(
                src_ref=source.at[peer], dst_ref=target.at[me],
                send_sem=side_send.at[kind], recv_sem=side_recv.at[kind],
                device_id=(peer // n_lo, lax.rem(peer, n_lo)), device_id_type=MESH,
            ).start()
            return carry

        lax.fori_loop(1, n, send, 0)
        target[me] = source[me]

    def settle(target, kind):
        all_but_one = target.at[pl.ds(0, n - 1)]
        pltpu.make_async_copy(all_but_one, all_but_one, side_recv.at[kind]).wait()

    def drain(source, kind):
        all_but_one = source.at[pl.ds(0, n - 1)]
        pltpu.make_async_copy(all_but_one, all_but_one, side_send.at[kind]).wait()

    def send_inv(step, carry):
        pltpu.make_async_remote_copy(
            src_ref=isend.at[0], dst_ref=irecv.at[me],
            send_sem=side_send.at[1], recv_sem=side_recv.at[1],
            device_id=other(step), device_id_type=MESH,
        ).start()
        return carry

    def forward(index, part, target_hi, target_lo):
        here = parts[part].at[index]
        pltpu.make_async_remote_copy(
            src_ref=here, dst_ref=here,
            send_sem=send_sem.at[part], recv_sem=recv_sem.at[part, index],
            device_id=(target_hi, target_lo), device_id_type=MESH,
        ).start()

    def arrive(index, part):
        here = parts[part].at[index]
        pltpu.make_async_copy(here, here, recv_sem.at[part, index]).wait()

    x_lo = lo + 1 - 2 * x
    y_hi = hi + CORES - 2 * CORES * y
    c_hi = hi + 1 - 2 * core

    def turned_z(step):
        return lax.rem(z + step, depth) * XDIM

    def send_own(part):
        forward(me, part, hi, x_lo)
        forward(me, part, y_hi, lo)
        for step in range(1, depth):
            forward(me, part, hi, turned_z(step) + x)
        forward(me, part, c_hi, lo)

    def column(part, step):
        if step == 0:
            return
        index = hi * n_lo + turned_z(step) + x
        arrive(index, part)
        forward(index, part, hi, x_lo)
        forward(index, part, y_hi, lo)
        forward(index, part, c_hi, lo)

    def beside(part, step):
        index = hi * n_lo + turned_z(step) + 1 - x
        arrive(index, part)
        if step % 2 == 0:
            forward(index, part, y_hi, lo)
        forward(index, part, c_hi, lo)
        index = y_hi * n_lo + turned_z(step) + x
        arrive(index, part)
        if step % 2 == 1:
            forward(index, part, hi, x_lo)
        forward(index, part, c_hi, lo)

    def corner(part, step):
        index = y_hi * n_lo + turned_z(step) + 1 - x
        arrive(index, part)
        forward(index, part, c_hi, lo)

    def relay(first, last):
        for t in range(first, last):
            for move, late in ((column, 0), (beside, LAG), (corner, 2 * LAG)):
                if 0 <= t - late < 3 * depth:
                    move((t - late) // depth, (t - late) % depth)
            if t == depth - 1:
                send_own(2)

    def from_core(part):
        for own_y in (True, False):
            base = (c_hi if own_y else lax.rem(c_hi + CORES, n_hi)) * n_lo
            for block in range(n_lo):
                arrive(base + block, part)

    exchange(xsend, xrecv, 0)
    lax.fori_loop(1, n, send_inv, 0)
    irecv[me] = isend[0]
    send_own(0)
    send_own(1)
    ready = depth + 2 * LAG
    relay(0, ready)
    from_core(0)
    settle(xrecv, 0)
    settle(irecv, 1)

    for pair in range(n // 2):
        at = slice(pair * 2 * rows, (pair + 1) * 2 * rows)
        one, two = xrecv[2 * pair], xrecv[2 * pair + 1]
        resid[0:half, at] = jnp.concatenate([one[:, :rows], two[:, :rows]], axis=1)
        resid[half:mine, at] = jnp.concatenate([one[:, rows:], two[:, rows:]], axis=1)
        low = lax.broadcasted_iota(jnp.int32, (1, 2 * rows), 1) < rows
        inv_row[:, at] = jnp.where(low, irecv[2 * pair], irecv[2 * pair + 1])

    group = n // 4
    span = group * rows

    def precondition():
        def down(q, carry):
            part = halves(resid[:, pl.ds(pl.multiple_of(q * span, span), span)], 0)
            for j in range(group):
                both = nn(part[:, j * rows : (j + 1) * rows], pay[q * group + j, :, 0:used])
                coef[q * group + j] = both[:mine] + both[mine:]
            return carry

        lax.fori_loop(0, n // group, down, 0)
        low = lax.broadcasted_iota(jnp.int32, (mine, 2 * rank), 1) < rank
        for chunk in range(used // (2 * rank)):
            at = slice(chunk * 2 * rank, (chunk + 1) * 2 * rank)
            first, second = 2 * chunk, 2 * chunk + 1
            if second == bits:
                total = coef[0, :, at]
                for k in range(1, n):
                    total = total + coef[k, :, at]
            for k in range(n):
                own = coef[k, :, at]
                left = own + coef[k ^ (1 << first), :, at]
                right = total if second == bits else own + coef[k ^ (1 << second), :, at]
                summed[k, :, at] = halves(jnp.where(low, left, right), 0)
        both = nn(summed[...].reshape(n * 2 * mine, used), couple[0]).reshape(n, 2 * mine, used)
        rest = nn(summed[:, :mine].reshape(n * mine, used), couple[1]).reshape(n, mine, used)
        lifted[...] = halves(both[:, :mine] + both[:, mine:] + rest, 1)

        def up(q, carry):
            pieces = []
            for j in range(group):
                both = nt(lifted[q * group + j], pay[q * group + j, :, 0:used])
                pieces.append(both[:mine] + both[mine:])
            at = pl.ds(pl.multiple_of(q * span, span), span)
            scaled[:, at] = inv_row[:, at] * resid[:, at] + jnp.concatenate(pieces, axis=1)
            return carry

        lax.fori_loop(0, n // group, up, 0)
        return jnp.sum(resid[...] * scaled[...], axis=1, keepdims=True)

    def apply_grm():
        cut = [direct[:, h * width : (h + 1) * width].astype(bf16) for h in range(n_hi)]
        total = [jnp.zeros((mine, width), f32) for _ in range(n_hi)]
        for h in range(n_hi):
            near, far = (h + 1) % n_hi, (h + 2) % n_hi
            base = h * n_lo
            full = near_pay[base : base + n_lo].reshape(width, width)
            total[h] = total[h] + nn(cut[h], full)
            full = next_pay[base : base + n_lo].reshape(width, width)
            total[h] = total[h] + nn(cut[near], full)
            total[near] = total[near] + nt(cut[h], full)
            sums = {}
            for r in range(2):
                q = r if h < CORES else 1 - r
                blocks = pay[
                    base + r * (n_lo // 2) : base + (r + 1) * (n_lo // 2), :, used : used + quad
                ].reshape(quad, quad)
                sums["h", q] = nn(cut[far][:, r * quad : (r + 1) * quad], blocks)
                sums["far", r] = nt(cut[h][:, q * quad : (q + 1) * quad], blocks)
            total[h] = total[h] + jnp.concatenate([sums["h", 0], sums["h", 1]], axis=1)
            total[far] = total[far] + jnp.concatenate([sums["far", 0], sums["far", 1]], axis=1)
        for h in range(n_hi):
            at = slice(h * width, (h + 1) * width)
            image[:, at] = var_ref[0] * total[h] + var_ref[1] * direct[:, at]

    energy = precondition()
    direct[...] = scaled[...]
    iterate[...] = jnp.zeros_like(iterate)
    relay(ready, 3 * depth + 2 * LAG)
    from_core(1)
    from_core(2)
    for step in range(ITERS):
        apply_grm()
        curvature = jnp.sum(direct[...] * image[...], axis=1, keepdims=True)
        alpha = jnp.where(steps_wanted > step, energy / curvature, 0.0)
        iterate[...] = iterate[...] + alpha * direct[...]
        resid[...] = resid[...] - alpha * image[...]
        if step + 1 < ITERS:
            fresh = precondition()
            direct[...] = scaled[...] + (fresh / energy) * direct[...]
            energy = fresh

    for which, field in ((0, iterate), (1, resid)):
        for pair in range(n // 2):
            both = field[:, pair * 2 * rows : (pair + 1) * 2 * rows]
            top, bottom = both[:half], both[half:]
            osend[2 * pair, which] = jnp.concatenate([top[:, :rows], bottom[:, :rows]], axis=1)
            osend[2 * pair + 1, which] = jnp.concatenate([top[:, rows:], bottom[:, rows:]], axis=1)
    exchange(osend, orecv, 2)
    for part in range(3):
        sent = parts[part].at[pl.ds(0, n - 1)]
        pltpu.make_async_copy(sent, sent, send_sem.at[part]).wait()
    drain(xsend, 0)
    drain(irecv, 1)
    settle(orecv, 2)
    for which, out_ref in ((0, sol_ref), (1, res_ref)):
        got = orecv[:, which]
        apart = jnp.concatenate([got[:, :, :rows], got[:, :, rows:]], axis=1)
        out_ref[...] = apart.reshape(columns, rows).T
    drain(osend, 2)


def run_whole(mesh, grm, right_sides, inv_diag, bases, couplings, level_map, variance, iters):
    n_hi, n_lo = mesh.shape["hi"], mesh.shape["lo"]
    n = n_hi * n_lo
    rows, columns = right_sides.shape
    mine = columns // n
    rank = couplings.shape[1]
    used = n.bit_length() * rank
    width = grm.shape[4]
    samples = rows * n
    f32, bf16 = jnp.float32, jnp.bfloat16
    vmem = pl.BlockSpec(memory_space=pltpu.VMEM)
    smem = pl.BlockSpec(memory_space=pltpu.SMEM)
    field = pltpu.VMEM((mine, samples), f32)
    tile = (mine // 2, 2 * rows)
    return pl.pallas_call(
        functools.partial(whole_kernel, n_hi, n_lo),
        out_shape=(jax.ShapeDtypeStruct((rows, columns), f32),) * 2,
        in_specs=[smem, smem] + [vmem] * 6,
        out_specs=(vmem, vmem),
        scratch_shapes=[
            pltpu.VMEM((n, rows, used + width // 2), bf16),
            pltpu.VMEM((n, rows, width), bf16),
            pltpu.VMEM((n, rows, width), bf16),
            pltpu.VMEM((n,) + tile, f32),
            pltpu.VMEM((n,) + tile, f32),
            pltpu.VMEM((1, 1, 2 * rows), f32),
            pltpu.VMEM((n, 1, 2 * rows), f32),
            pltpu.VMEM((n, 2) + tile, f32),
            pltpu.VMEM((n, 2) + tile, f32),
            field, field, field, field, field,
            pltpu.VMEM((1, samples), f32),
            pltpu.VMEM((n, mine, used), f32),
            pltpu.VMEM((n, 2 * mine, used), bf16),
            pltpu.VMEM((n, 2 * mine, used), bf16),
            pltpu.VMEM((2, used, used), bf16),
            pltpu.SemaphoreType.DMA((3,)),
            pltpu.SemaphoreType.DMA((3, n)),
            pltpu.SemaphoreType.DMA((3,)),
            pltpu.SemaphoreType.DMA((3,)),
        ],
        compiler_params=pltpu.CompilerParams(
            collective_id=0, has_side_effects=True, vmem_limit_bytes=56 * 2**20
        ),
    )(
        variance, level_map,
        grm.reshape(grm.shape[0], rows, width), right_sides, inv_diag.reshape(1, rows),
        bases, couplings, iters.reshape(1, columns),
    )


def solution(mesh):
    in_specs = (
        P(None, "lo", None, "hi", None),
        P(("hi", "lo"), None),
        P(("hi", "lo")),
        P(("hi", "lo"), None),
        P(),
        P(),
        P(),
        P(),
    )
    out_specs = (P(("hi", "lo"), None), P(("hi", "lo"), None))

    def program(*arrays):
        body = local
        if fits_one_device(mesh, arrays[0], arrays[1], arrays[3], arrays[4]):
            body = functools.partial(run_whole, mesh)
        return jax.shard_map(
            body, mesh=mesh, in_specs=in_specs, out_specs=out_specs, check_vma=False
        )(*arrays)

    return program
```

```python
import functools

import jax
import jax.numpy as jnp
from jax import lax
from jax.experimental import pallas as pl
from jax.experimental.pallas import tpu as pltpu
from jax.sharding import PartitionSpec as P

ITERS = 3
MESH = pl.DeviceIdType.MESH


def from_partner(value, axis, bit):
    mask = 2**bit
    pairs = [(source, source ^ mask) for source in range(lax.axis_size(axis))]
    return lax.ppermute(value, axis, pairs)


def level_pieces(coefficients, couplings, level):
    level_ids = jnp.arange(couplings.shape[0], dtype=jnp.int32)
    select = (level_ids == level).astype(jnp.float32)
    own_part = jnp.einsum("l,lrb->rb", select, coefficients)
    matrix = jnp.einsum("l,lrs->rs", select, couplings)
    return (own_part, matrix, select)


def add_level(stacked, own_part, other_part, matrix, select):
    term = jnp.dot(matrix, own_part + other_part, precision=lax.Precision.HIGHEST)
    return stacked + select[:, None, None] * term[None]


def local(grm, right_sides, inv_diag, bases, couplings, level_map, variance, iters_per_column):
    row_count, column_count = right_sides.shape
    grm_block = grm.reshape(-1, grm.shape[4])
    level_total = couplings.shape[0]
    rank_width = couplings.shape[1]
    lo_bits = lax.axis_size("lo").bit_length() - 1
    hi_bits = lax.axis_size("hi").bit_length() - 1
    genetic = variance[0]
    noise = variance[1]

    def precondition(resid):
        coefficients = lax.dot_general(
            bases, resid, (((0,), (0,)), ((), ())), precision=lax.Precision.HIGHEST
        )
        coefficients = coefficients.reshape(level_total, rank_width, column_count)
        stacked = jnp.zeros((level_total - 1, rank_width, column_count), jnp.float32)
        for bit_index in range(lo_bits):
            own_part, matrix, select = level_pieces(coefficients, couplings, level_map[bit_index])
            other_part = from_partner(own_part.astype(jnp.bfloat16), "lo", bit_index).astype(
                own_part.dtype
            )
            stacked = add_level(stacked, own_part, other_part, matrix, select[: level_total - 1])
        for bit_index in range(hi_bits):
            own_part, matrix, select = level_pieces(
                coefficients, couplings, level_map[lo_bits + bit_index]
            )
            other_part = from_partner(own_part.astype(jnp.bfloat16), "hi", bit_index).astype(
                own_part.dtype
            )
            stacked = add_level(stacked, own_part, other_part, matrix, select[: level_total - 1])
        split_at = (level_total - 1) * rank_width
        local_part = inv_diag[:, None] * resid + jnp.dot(
            bases[:, :split_at],
            stacked.reshape(split_at, column_count),
            precision=lax.Precision.HIGHEST,
        )
        coarse_basis = bases[:, split_at:]
        partial_energy = jnp.sum(resid * local_part, axis=0)
        total, summed_energy = lax.psum(
            (coefficients[level_total - 1], partial_energy), ("hi", "lo")
        )
        coarse = jnp.dot(couplings[level_total - 1], total, precision=lax.Precision.HIGHEST)
        scaled = local_part + jnp.dot(coarse_basis, coarse, precision=lax.Precision.HIGHEST)
        energy = summed_energy + jnp.sum(total * coarse, axis=0)
        return (scaled, energy)

    solution = jnp.zeros_like(right_sides)
    residual = right_sides
    scaled, energy = precondition(residual)
    direction = scaled
    for step in range(ITERS):
        rounded = direction.astype(jnp.bfloat16)
        partial_value = jnp.dot(
            grm_block,
            lax.all_gather(rounded, "lo", axis=0, tiled=True),
            preferred_element_type=jnp.float32,
        )
        product = lax.psum_scatter(partial_value, "hi", scatter_dimension=0, tiled=True)
        image = genetic * product + noise * direction
        curvature = lax.psum(jnp.sum(direction * image, axis=0), ("hi", "lo"))
        alpha = energy / curvature
        stepsize = jnp.where(step < iters_per_column, alpha, jnp.zeros_like(alpha))
        solution = solution + stepsize * direction
        residual = residual - stepsize * image
        if step + 1 < ITERS:
            scaled, fresh = precondition(residual)
            direction = scaled + fresh / energy * direction
            energy = fresh
    return (solution, residual)


def fits_one_device(mesh, grm, right_sides, bases, couplings):
    n_hi, n_lo = mesh.shape["hi"], mesh.shape["lo"]
    devices = n_hi * n_lo
    samples, columns = right_sides.shape
    rank = couplings.shape[1]
    bits = devices.bit_length() - 1
    used = (bits + 1) * rank
    width = samples // n_hi
    return (
        n_hi == 2 * CORES
        and n_lo % (2 * XDIM) == 0
        and columns % (16 * devices) == 0
        and columns // devices == 16
        and used % 128 == 0
        and (bits + 1) % 2 == 0
        and width % 256 == 0
        and 2 * rank == 128
        and 2 * (samples // devices) == 128
        and samples * (samples + used) * 2 < 2**24
    )


CORES = 2
XDIM = 2
LAG = 4


def nt(a, b):
    return lax.dot_general(a, b, (((1,), (1,)), ((), ())), preferred_element_type=jnp.float32)


def nn(a, b):
    return jnp.dot(a, b, preferred_element_type=jnp.float32)


def halves(value, axis):
    top = value.astype(jnp.bfloat16)
    rest = (value - top.astype(jnp.float32)).astype(jnp.bfloat16)
    return jnp.concatenate([top, rest], axis=axis)


def whole_kernel(
    n_hi, n_lo,
    var_ref, level_ref,
    grm_ref, rhs_ref, inv_ref, bases_ref, coup_ref, iters_ref,
    sol_ref, res_ref,
    pay, near_pay, next_pay, xsend, xrecv, isend, irecv, osend, orecv,
    resid, direct, image, iterate, scaled, inv_row,
    coef, summed, lifted, couple,
    send_sem, recv_sem, side_send, side_recv,
):
    hi, lo = lax.axis_index("hi"), lax.axis_index("lo")
    n = n_hi * n_lo
    me = hi * n_lo + lo
    y, core = hi // CORES, hi % CORES
    z, x = lo // XDIM, lo % XDIM
    depth = n_lo // XDIM
    rows, columns = rhs_ref.shape
    mine = columns // n
    half = mine // 2
    levels = coup_ref.shape[0]
    rank = coup_ref.shape[1]
    bits = n.bit_length() - 1
    used = (bits + 1) * rank
    width = grm_ref.shape[2]
    quad = width // 2
    samples = rows * n
    f32, bf16 = jnp.float32, jnp.bfloat16

    barrier = pltpu.get_barrier_semaphore()

    def other(step):
        peer = lax.rem(me + step, n)
        return (peer // n_lo, lax.rem(peer, n_lo))

    def greet(step, carry):
        pl.semaphore_signal(barrier, inc=1, device_id=other(step), device_id_type=MESH)
        return carry

    lax.fori_loop(1, n, greet, 0)

    column_id = lax.broadcasted_iota(jnp.int32, (1, used), 1)
    wanted = jnp.full((1, used), (levels - 1) * rank, jnp.int32)
    for bit in range(bits):
        wanted = jnp.where(column_id // rank == bit, level_ref[bit] * rank, wanted)
    wanted = wanted + column_id % rank
    pick = lax.broadcasted_iota(jnp.int32, (levels * rank, used), 0) == wanted
    own_bases = nn(bases_ref[...].astype(bf16), pick.astype(f32).astype(bf16))
    parts = (pay, near_pay, next_pay)
    pay[me, :, 0:used] = own_bases.astype(bf16)
    across = lax.rem(hi + CORES, n_hi)
    upper = jnp.where(hi < CORES, lo >= n_lo // 2, lo < n_lo // 2)
    both = grm_ref[across]
    pay[me, :, used : used + quad] = jnp.where(
        upper, both[:, quad:].astype(f32), both[:, :quad].astype(f32)
    ).astype(bf16)
    near_pay[me] = grm_ref[hi]
    next_pay[me] = grm_ref[lax.rem(hi + 1, n_hi)]

    turned = rhs_ref[...].T.reshape(n, mine, rows)
    xsend[...] = jnp.concatenate([turned[:, :half], turned[:, half:]], axis=2)
    isend[0, :, 0:rows] = inv_ref[...]
    isend[0, :, rows:] = inv_ref[...]

    couple[...] = jnp.zeros_like(couple)
    for bit in range(bits + 1):
        block = coup_ref[level_ref[bit]] if bit < bits else coup_ref[levels - 1]
        at = slice(bit * rank, (bit + 1) * rank)
        couple[0, at, at] = block.astype(bf16)
        couple[1, at, at] = (block - block.astype(bf16).astype(f32)).astype(bf16)
    taken = lax.broadcasted_iota(jnp.int32, (mine, columns), 1) == (
        me * mine + lax.broadcasted_iota(jnp.int32, (mine, columns), 0)
    )
    steps_wanted = jnp.sum(
        jnp.where(taken, iters_ref[...].astype(f32), 0.0), axis=1, keepdims=True
    )

    pl.semaphore_wait(barrier, n - 1)

    def exchange(source, target, kind):
        def send(step, carry):
            peer = lax.rem(me + step, n)
            pltpu.make_async_remote_copy(
                src_ref=source.at[peer], dst_ref=target.at[me],
                send_sem=side_send.at[kind], recv_sem=side_recv.at[kind],
                device_id=(peer // n_lo, lax.rem(peer, n_lo)), device_id_type=MESH,
            ).start()
            return carry

        lax.fori_loop(1, n, send, 0)
        target[me] = source[me]

    def exchange_field(which):
        def send(step, carry):
            peer = lax.rem(me + step, n)
            pltpu.make_async_remote_copy(
                src_ref=osend.at[peer, which], dst_ref=orecv.at[me, which],
                send_sem=side_send.at[2 + which], recv_sem=side_recv.at[2 + which],
                device_id=(peer // n_lo, lax.rem(peer, n_lo)), device_id_type=MESH,
            ).start()
            return carry

        lax.fori_loop(1, n, send, 0)
        orecv[me, which] = osend[me, which]

    def settle(target, kind):
        all_but_one = target.at[pl.ds(0, n - 1)]
        pltpu.make_async_copy(all_but_one, all_but_one, side_recv.at[kind]).wait()

    def drain(source, kind):
        all_but_one = source.at[pl.ds(0, n - 1)]
        pltpu.make_async_copy(all_but_one, all_but_one, side_send.at[kind]).wait()

    def send_inv(step, carry):
        pltpu.make_async_remote_copy(
            src_ref=isend.at[0], dst_ref=irecv.at[me],
            send_sem=side_send.at[1], recv_sem=side_recv.at[1],
            device_id=other(step), device_id_type=MESH,
        ).start()
        return carry

    def forward(index, part, target_hi, target_lo):
        here = parts[part].at[index]
        pltpu.make_async_remote_copy(
            src_ref=here, dst_ref=here,
            send_sem=send_sem.at[part], recv_sem=recv_sem.at[part, index],
            device_id=(target_hi, target_lo), device_id_type=MESH,
        ).start()

    def arrive(index, part):
        here = parts[part].at[index]
        pltpu.make_async_copy(here, here, recv_sem.at[part, index]).wait()

    x_lo = lo + 1 - 2 * x
    y_hi = hi + CORES - 2 * CORES * y
    c_hi = hi + 1 - 2 * core

    def turned_z(step):
        return lax.rem(z + step, depth) * XDIM

    def send_own(part):
        forward(me, part, hi, x_lo)
        forward(me, part, y_hi, lo)
        for step in range(1, depth):
            forward(me, part, hi, turned_z(step) + x)
        forward(me, part, c_hi, lo)

    def column(part, step):
        if step == 0:
            return
        index = hi * n_lo + turned_z(step) + x
        arrive(index, part)
        forward(index, part, hi, x_lo)
        forward(index, part, y_hi, lo)
        forward(index, part, c_hi, lo)

    def beside(part, step):
        index = hi * n_lo + turned_z(step) + 1 - x
        arrive(index, part)
        if step % 2 == 0:
            forward(index, part, y_hi, lo)
        forward(index, part, c_hi, lo)
        index = y_hi * n_lo + turned_z(step) + x
        arrive(index, part)
        if step % 2 == 1:
            forward(index, part, hi, x_lo)
        forward(index, part, c_hi, lo)

    def corner(part, step):
        index = y_hi * n_lo + turned_z(step) + 1 - x
        arrive(index, part)
        forward(index, part, c_hi, lo)

    def relay(first, last):
        for t in range(first, last):
            for move, late in ((column, 0), (beside, LAG), (corner, 2 * LAG)):
                if 0 <= t - late < 3 * depth:
                    move((t - late) // depth, (t - late) % depth)
            if t == depth - 1:
                send_own(2)

    def from_core(part):
        for own_y in (True, False):
            base = (c_hi if own_y else lax.rem(c_hi + CORES, n_hi)) * n_lo
            for block in range(n_lo):
                arrive(base + block, part)

    send_own(0)
    exchange(xsend, xrecv, 0)
    lax.fori_loop(1, n, send_inv, 0)
    irecv[me] = isend[0]
    send_own(1)
    ready = depth + 2 * LAG
    relay(0, ready)
    from_core(0)
    settle(xrecv, 0)
    settle(irecv, 1)

    for pair in range(n // 2):
        at = slice(pair * 2 * rows, (pair + 1) * 2 * rows)
        one, two = xrecv[2 * pair], xrecv[2 * pair + 1]
        resid[0:half, at] = jnp.concatenate([one[:, :rows], two[:, :rows]], axis=1)
        resid[half:mine, at] = jnp.concatenate([one[:, rows:], two[:, rows:]], axis=1)
        low = lax.broadcasted_iota(jnp.int32, (1, 2 * rows), 1) < rows
        inv_row[:, at] = jnp.where(low, irecv[2 * pair], irecv[2 * pair + 1])

    group = n // 4
    span = group * rows

    def precondition():
        def down(q, carry):
            part = halves(resid[:, pl.ds(pl.multiple_of(q * span, span), span)], 0)
            for j in range(group):
                both = nn(part[:, j * rows : (j + 1) * rows], pay[q * group + j, :, 0:used])
                coef[q * group + j] = both[:mine] + both[mine:]
            return carry

        lax.fori_loop(0, n // group, down, 0)
        low = lax.broadcasted_iota(jnp.int32, (mine, 2 * rank), 1) < rank
        for chunk in range(used // (2 * rank)):
            at = slice(chunk * 2 * rank, (chunk + 1) * 2 * rank)
            first, second = 2 * chunk, 2 * chunk + 1
            if second == bits:
                total = coef[0, :, at]
                for k in range(1, n):
                    total = total + coef[k, :, at]
            for k in range(n):
                own = coef[k, :, at]
                left = own + coef[k ^ (1 << first), :, at]
                right = total if second == bits else own + coef[k ^ (1 << second), :, at]
                summed[k, :, at] = halves(jnp.where(low, left, right), 0)
        both = nn(summed[...].reshape(n * 2 * mine, used), couple[0]).reshape(n, 2 * mine, used)
        rest = nn(summed[:, :mine].reshape(n * mine, used), couple[1]).reshape(n, mine, used)
        lifted[...] = halves(both[:, :mine] + both[:, mine:] + rest, 1)

        def up(q, carry):
            pieces = []
            for j in range(group):
                both = nt(lifted[q * group + j], pay[q * group + j, :, 0:used])
                pieces.append(both[:mine] + both[mine:])
            at = pl.ds(pl.multiple_of(q * span, span), span)
            scaled[:, at] = inv_row[:, at] * resid[:, at] + jnp.concatenate(pieces, axis=1)
            return carry

        lax.fori_loop(0, n // group, up, 0)
        return jnp.sum(resid[...] * scaled[...], axis=1, keepdims=True)

    def apply_grm():
        cut = [direct[:, h * width : (h + 1) * width].astype(bf16) for h in range(n_hi)]
        total = [jnp.zeros((mine, width), f32) for _ in range(n_hi)]
        for h in range(n_hi):
            near, far = (h + 1) % n_hi, (h + 2) % n_hi
            base = h * n_lo
            full = near_pay[base : base + n_lo].reshape(width, width)
            total[h] = total[h] + nn(cut[h], full)
            full = next_pay[base : base + n_lo].reshape(width, width)
            total[h] = total[h] + nn(cut[near], full)
            total[near] = total[near] + nt(cut[h], full)
            sums = {}
            for r in range(2):
                q = r if h < CORES else 1 - r
                blocks = pay[
                    base + r * (n_lo // 2) : base + (r + 1) * (n_lo // 2), :, used : used + quad
                ].reshape(quad, quad)
                sums["h", q] = nn(cut[far][:, r * quad : (r + 1) * quad], blocks)
                sums["far", r] = nt(cut[h][:, q * quad : (q + 1) * quad], blocks)
            total[h] = total[h] + jnp.concatenate([sums["h", 0], sums["h", 1]], axis=1)
            total[far] = total[far] + jnp.concatenate([sums["far", 0], sums["far", 1]], axis=1)
        for h in range(n_hi):
            at = slice(h * width, (h + 1) * width)
            image[:, at] = var_ref[0] * total[h] + var_ref[1] * direct[:, at]

    energy = precondition()
    direct[...] = scaled[...]
    iterate[...] = jnp.zeros_like(iterate)
    relay(ready, 3 * depth + 2 * LAG)
    from_core(1)
    from_core(2)
    for step in range(ITERS):
        apply_grm()
        curvature = jnp.sum(direct[...] * image[...], axis=1, keepdims=True)
        alpha = jnp.where(steps_wanted > step, energy / curvature, 0.0)
        iterate[...] = iterate[...] + alpha * direct[...]
        resid[...] = resid[...] - alpha * image[...]
        if step + 1 < ITERS:
            fresh = precondition()
            direct[...] = scaled[...] + (fresh / energy) * direct[...]
            energy = fresh

    for which, field in ((0, iterate), (1, resid)):
        for pair in range(n // 2):
            both = field[:, pair * 2 * rows : (pair + 1) * 2 * rows]
            top, bottom = both[:half], both[half:]
            osend[2 * pair, which] = jnp.concatenate([top[:, :rows], bottom[:, :rows]], axis=1)
            osend[2 * pair + 1, which] = jnp.concatenate([top[:, rows:], bottom[:, rows:]], axis=1)
        exchange_field(which)
    for part in range(3):
        sent = parts[part].at[pl.ds(0, n - 1)]
        pltpu.make_async_copy(sent, sent, send_sem.at[part]).wait()
    drain(xsend, 0)
    drain(irecv, 1)
    for which, out_ref in ((0, sol_ref), (1, res_ref)):
        settle(orecv.at[:, which], 2 + which)
        got = orecv[:, which]
        apart = jnp.concatenate([got[:, :, :rows], got[:, :, rows:]], axis=1)
        out_ref[...] = apart.reshape(columns, rows).T
    for which in range(2):
        drain(osend.at[:, which], 2 + which)


def run_whole(mesh, grm, right_sides, inv_diag, bases, couplings, level_map, variance, iters):
    n_hi, n_lo = mesh.shape["hi"], mesh.shape["lo"]
    n = n_hi * n_lo
    rows, columns = right_sides.shape
    mine = columns // n
    rank = couplings.shape[1]
    used = n.bit_length() * rank
    width = grm.shape[4]
    samples = rows * n
    f32, bf16 = jnp.float32, jnp.bfloat16
    vmem = pl.BlockSpec(memory_space=pltpu.VMEM)
    smem = pl.BlockSpec(memory_space=pltpu.SMEM)
    field = pltpu.VMEM((mine, samples), f32)
    tile = (mine // 2, 2 * rows)
    return pl.pallas_call(
        functools.partial(whole_kernel, n_hi, n_lo),
        out_shape=(jax.ShapeDtypeStruct((rows, columns), f32),) * 2,
        in_specs=[smem, smem] + [vmem] * 6,
        out_specs=(vmem, vmem),
        scratch_shapes=[
            pltpu.VMEM((n, rows, used + width // 2), bf16),
            pltpu.VMEM((n, rows, width), bf16),
            pltpu.VMEM((n, rows, width), bf16),
            pltpu.VMEM((n,) + tile, f32),
            pltpu.VMEM((n,) + tile, f32),
            pltpu.VMEM((1, 1, 2 * rows), f32),
            pltpu.VMEM((n, 1, 2 * rows), f32),
            pltpu.VMEM((n, 2) + tile, f32),
            pltpu.VMEM((n, 2) + tile, f32),
            field, field, field, field, field,
            pltpu.VMEM((1, samples), f32),
            pltpu.VMEM((n, mine, used), f32),
            pltpu.VMEM((n, 2 * mine, used), bf16),
            pltpu.VMEM((n, 2 * mine, used), bf16),
            pltpu.VMEM((2, used, used), bf16),
            pltpu.SemaphoreType.DMA((3,)),
            pltpu.SemaphoreType.DMA((3, n)),
            pltpu.SemaphoreType.DMA((4,)),
            pltpu.SemaphoreType.DMA((4,)),
        ],
        compiler_params=pltpu.CompilerParams(
            collective_id=0, has_side_effects=True, vmem_limit_bytes=56 * 2**20
        ),
    )(
        variance, level_map,
        grm.reshape(grm.shape[0], rows, width), right_sides, inv_diag.reshape(1, rows),
        bases, couplings, iters.reshape(1, columns),
    )


def solution(mesh):
    in_specs = (
        P(None, "lo", None, "hi", None),
        P(("hi", "lo"), None),
        P(("hi", "lo")),
        P(("hi", "lo"), None),
        P(),
        P(),
        P(),
        P(),
    )
    out_specs = (P(("hi", "lo"), None), P(("hi", "lo"), None))

    def program(*arrays):
        body = local
        if fits_one_device(mesh, arrays[0], arrays[1], arrays[3], arrays[4]):
            body = functools.partial(run_whole, mesh)
        return jax.shard_map(
            body, mesh=mesh, in_specs=in_specs, out_specs=out_specs, check_vma=False
        )(*arrays)

    return program
```
